32 devices in a mesh: groups: 2 (over x), ep: 8 (over z, y), tp: 2 (over core).
Axes of the slice: x: 2, y: 2, z: 4, core: 2. Of those that a mesh axis runs over, the one named last changes fastest.
Arguments:
- hidden: bfloat16 [256, 3584], P(('groups', 'ep'), 'tp'), parts along dimension 0, may hold values from -6 to 6
- routes: int32 [256, 4], P(('groups', 'ep')), parts along dimension 0, may hold values from 0 to 7, as said below
- router_weight: bfloat16 [3584, 8], P('tp'), may hold values from -0.1875 to 0.1875
- gate_weight: bfloat16 [8, 3584, 1024], P('ep', None, 'tp'), may hold values from -0.09375 to 0.09375
- up_weight: bfloat16 [8, 3584, 1024], P('ep', None, 'tp'), may hold values from -0.09375 to 0.09375
- down_weight: bfloat16 [8, 1024, 3584], P('ep', 'tp'), may hold values from -0.1875 to 0.1875
- q_latent: bfloat16 [64, 64, 512], P(('groups', 'ep'), 'tp'), parts along dimension 0, may hold values from -48 to 48
- q_rope: bfloat16 [64, 64, 64], P(('groups', 'ep'), 'tp'), parts along dimension 0, may hold values from -48 to 48
- cache_latent: bfloat16 [64, 256, 512], P(('groups', 'ep')), parts along dimension 0, may hold values from -4 to 4
- cache_rope: bfloat16 [64, 64, 256], P(('groups', 'ep')), parts along dimension 0, may hold values from -4 to 4
- lengths: int32 [64], P(('groups', 'ep')), parts along dimension 0, may hold values from 16 to 256, as said below
Outputs:
- moe_out: bfloat16 [256, 3584], P(('groups', 'ep'), 'tp'), parts along dimension 0
- attn_latent: bfloat16 [64, 64, 512], P(('groups', 'ep'), 'tp'), parts along dimension 0
The draws below stay inside these ranges and needn't reach their ends.
There are 2 independent parts, one for each index of `groups`. The reference program is written for one: setup_inputs(seed, part) draws one part's arguments, and reference() takes and returns one part's arrays. A program takes and returns all parts, laid end to end along the dimension named above; an argument that names none is the same for every part. Nothing has to cross between parts.
Inputs may be any that keep to these rules, and one draw needn't show every extreme that they name: `routes`: each row names 4 different experts; in each aligned block of 16 rows (the rows of one index of ep) no expert is named more than 16 times, and one expert, the same in every block, is named exactly 16 times in each block. `lengths`: one sequence has 256 live positions and one has 16.
All inputs are finite; a program needn't handle non-finite values.
Results may differ from the reference program's by a relative error of at most 0.0085.
Values may be sent and summed in bfloat16 or wider, within the bound.
A program may use at most 128 MiB of HBM per device.

```python
import jax
import jax.numpy as jnp
from jax import lax

D = 3584
FFW = 1024
LAT = 512
ROPE = 64
HEADS = 64
TOK_DEV = 16
CACHE = 256
EXPERTS = 8
TOP = 4
CAP = 16
TOKENS = 128
SEQS = 32


def cache_parts(key):
    latent_key, rope_key = jax.random.split(jax.random.fold_in(key, 7))
    latent = jnp.clip(jax.random.normal(latent_key, (SEQS, CACHE, LAT), jnp.float32), -4.0, 4.0)
    rotary = jnp.clip(jax.random.normal(rope_key, (SEQS, ROPE, CACHE), jnp.float32), -4.0, 4.0)
    return (latent.astype(jnp.bfloat16).astype(jnp.float32), rotary.astype(jnp.bfloat16).astype(jnp.float32))


def query_parts(key):
    query_key = jax.random.fold_in(key, 13)
    keys = jax.random.split(query_key, 1)
    query_bound = 48.0 * 576.0 / (LAT + ROPE)
    queries = jnp.clip(1.15 * jax.random.normal(keys[0], (SEQS, HEADS, LAT + ROPE), jnp.float32), -5.0, 5.0)
    queries = jnp.clip(queries, -query_bound, query_bound)
    return (queries[:, :, :LAT], queries[:, :, LAT:])


def draw_q_latent(key, part):
    return query_parts(key)[0].astype(jnp.bfloat16)


def draw_q_rope(key, part):
    return query_parts(key)[1].astype(jnp.bfloat16)


def draw_cache_latent(key, part):
    return cache_parts(key)[0].astype(jnp.bfloat16)


def draw_cache_rope(key, part):
    return cache_parts(key)[1].astype(jnp.bfloat16)


def draw_lengths(key, part):
    keys = jax.random.split(jax.random.fold_in(key, 3), 3)
    shortest_len = CACHE // 16
    drawn_lengths = jax.random.randint(keys[0], (SEQS,), shortest_len, CACHE + 1, dtype=jnp.int32)
    longest_at = jax.random.randint(keys[1], (), 0, SEQS, dtype=jnp.int32)
    shortest_at = (longest_at + 1 + jax.random.randint(keys[2], (), 0, SEQS - 1, dtype=jnp.int32)) % SEQS
    drawn_lengths = drawn_lengths.at[longest_at].set(CACHE).at[shortest_at].set(shortest_len)
    return drawn_lengths.astype(jnp.int32)


def draw_routes(key, part):
    block_count = TOKENS // TOK_DEV
    others = EXPERTS - 1
    remaining = TOK_DEV * TOP - CAP
    base_load = remaining // others
    extra_count = remaining % others
    pair_count = others // 2
    reach = min(base_load, CAP - base_load - 1)
    keys = jax.random.split(jax.random.fold_in(key, 5), 3)
    expert_order = jax.random.permutation(keys[0], EXPERTS).astype(jnp.int32)
    shifts = jax.random.randint(keys[1], (block_count, pair_count), 0, reach + 1, dtype=jnp.int32)
    other_loads = base_load + (jnp.arange(others, dtype=jnp.int32) < extra_count).astype(jnp.int32)
    other_loads = jnp.broadcast_to(other_loads[None, :], (block_count, others))
    other_loads = other_loads.at[:, 0:2 * pair_count:2].add(-shifts)
    other_loads = other_loads.at[:, 1:2 * pair_count:2].add(shifts)
    loads = jnp.concatenate([jnp.full((block_count, 1), CAP, jnp.int32), other_loads], axis=1)
    ends = jnp.cumsum(loads, axis=1).astype(jnp.int32)
    position = jnp.arange(TOK_DEV * TOP, dtype=jnp.int32)
    which = jnp.sum((position[None, :, None] >= ends[:, None, :]).astype(jnp.int32), axis=2)
    listed = expert_order[which]
    table = jnp.transpose(listed.reshape(block_count, TOP, TOK_DEV), (0, 2, 1))
    token_perms = jax.vmap(lambda sub_key: jax.random.permutation(sub_key, TOK_DEV))(jax.random.split(keys[2], block_count))
    table = jax.vmap(lambda rows_table, perm_order: rows_table[perm_order])(table, token_perms)
    return table.reshape(TOKENS, TOP).astype(jnp.int32)


def levels(key, shape, cuts, low, top_value):
    def one(axis_at, shards_of):
        steps = jax.random.uniform(jax.random.fold_in(jax.random.fold_in(key, 6), axis_at), (shards_of,), jnp.float32, low / len(cuts), top_value / len(cuts))
        return jnp.repeat(jnp.exp(steps), shape[axis_at] // shards_of).reshape((-1,) + (1,) * (len(shape) - axis_at - 1))

    gain = one(*cuts[0])
    for cut in cuts[1:]:
        gain = gain * one(*cut)
    return gain


def normal_values(key, extent, scale, bound, cuts=(), kind=jnp.bfloat16):
    entries = jax.random.normal(key, extent, jnp.float32) * scale
    if len(cuts) > 0:
        entries = levels(key, extent, cuts, -0.22, 0.18) * entries
    return jnp.clip(entries, min=-bound, max=bound).astype(kind)


def setup_inputs(seed: int = 0, part: int = 0) -> dict:
    streams_of = jax.random.split(jax.random.key(seed), 12)
    own_keys = jax.random.split(jax.random.fold_in(streams_of[11], part), 12)
    return {
        "hidden": normal_values(own_keys[0], (TOKENS, D), 1.0, 6.0, ((0, 8), (1, 2))),
        "routes": draw_routes(jax.random.fold_in(jax.random.fold_in(streams_of[11], part), 71), part),
        "router_weight": normal_values(streams_of[2], (D, EXPERTS), (D // 4) ** -0.5, 0.1875, ((0, 2),)),
        "gate_weight": normal_values(streams_of[3], (EXPERTS, D, FFW), D ** -0.5, 0.09375, ((0, 8), (2, 2))),
        "up_weight": normal_values(streams_of[4], (EXPERTS, D, FFW), D ** -0.5, 0.09375, ((0, 8), (2, 2))),
        "down_weight": normal_values(streams_of[5], (EXPERTS, FFW, D), FFW ** -0.5, 0.1875, ((0, 8), (1, 2))),
        "q_latent": draw_q_latent(jax.random.fold_in(jax.random.fold_in(streams_of[11], part), 71), part),
        "q_rope": draw_q_rope(jax.random.fold_in(jax.random.fold_in(streams_of[11], part), 71), part),
        "cache_latent": draw_cache_latent(jax.random.fold_in(jax.random.fold_in(streams_of[11], part), 71), part),
        "cache_rope": draw_cache_rope(jax.random.fold_in(jax.random.fold_in(streams_of[11], part), 71), part),
        "lengths": draw_lengths(jax.random.fold_in(jax.random.fold_in(streams_of[11], part), 71), part),
    }


softmax_scale = 192.0 ** -0.5
routed_scale = 2.5
block_rows = 32


def expert_block(hidden, gate_weight, up_weight, down_weight, token_index, expert_index):
    picked = jnp.take(hidden, token_index, axis=0)
    gate_part = jnp.dot(picked, gate_weight[expert_index], preferred_element_type=jnp.float32)
    up_part = jnp.dot(picked, up_weight[expert_index], preferred_element_type=jnp.float32)
    active = (jax.nn.silu(gate_part) * up_part).astype(jnp.bfloat16)
    return jnp.dot(active, down_weight[expert_index], preferred_element_type=jnp.float32).astype(jnp.bfloat16)


def routed_rows(hidden, routes, gate_weight, up_weight, down_weight):
    total = TOKENS * TOP
    block_count = (total + block_rows - 1) // block_rows + EXPERTS
    flat_ids = routes.reshape(-1).astype(jnp.int32)
    order = jnp.argsort(flat_ids, stable=True).astype(jnp.int32)
    counts = jnp.zeros((EXPERTS,), jnp.int32).at[flat_ids].add(1)
    padded = ((counts + block_rows - 1) // block_rows * block_rows).astype(jnp.int32)
    padded_end = jnp.cumsum(padded).astype(jnp.int32)
    padded_start = (padded_end - padded).astype(jnp.int32)
    seg_start = (jnp.cumsum(counts) - counts).astype(jnp.int32)
    sorted_ids = flat_ids[order]
    within = jnp.arange(total, dtype=jnp.int32) - seg_start[sorted_ids]
    target = (padded_start[sorted_ids] + within).astype(jnp.int32)
    token_of = jnp.zeros((block_count * block_rows,), jnp.int32).at[target].set((order // TOP).astype(jnp.int32))
    block_start = jnp.arange(block_count, dtype=jnp.int32) * block_rows
    block_expert = jnp.sum((block_start[:, None] >= padded_end[None, :]).astype(jnp.int32), axis=1).astype(jnp.int32)
    block_expert = jnp.minimum(block_expert, EXPERTS - 1).astype(jnp.int32)

    def one_block(item):
        token_index, expert_index = item
        return expert_block(hidden, gate_weight, up_weight, down_weight, token_index, expert_index)

    outputs = lax.map(one_block, (token_of.reshape(block_count, block_rows), block_expert))
    outputs = outputs.reshape(block_count * block_rows, D)
    slot_of = jnp.zeros((total,), jnp.int32).at[order].set(target)
    return jnp.take(outputs, slot_of, axis=0).reshape(TOKENS, TOP, D)


def attention(q_latent, q_rope, cache_latent, cache_rope, lengths):
    scores = jnp.einsum("bhl,bjl->bhj", q_latent.astype(jnp.float32), cache_latent.astype(jnp.float32))
    scores = scores + jnp.einsum("bhr,brj->bhj", q_rope.astype(jnp.float32), cache_rope.astype(jnp.float32))
    scores = scores * softmax_scale
    position = jnp.arange(CACHE, dtype=jnp.int32)
    live = position[None, None, :] < lengths.astype(jnp.int32)[:, None, None]
    scores = jnp.where(live, scores, -jnp.inf)
    highest = jnp.max(scores, axis=2, keepdims=True)
    expo = jnp.where(live, jnp.exp(scores - highest), 0.0)
    probs = (expo / jnp.sum(expo, axis=2, keepdims=True)).astype(jnp.bfloat16)
    mixed = jnp.einsum("bhj,bjl->bhl", probs.astype(jnp.float32), cache_latent.astype(jnp.float32))
    return mixed.astype(jnp.bfloat16)


def reference(hidden, routes, router_weight, gate_weight, up_weight, down_weight, q_latent, q_rope, cache_latent, cache_rope, lengths):
    logits = jnp.dot(hidden, router_weight, preferred_element_type=jnp.float32)
    affinity = jax.nn.sigmoid(logits)
    chosen = jnp.take_along_axis(affinity, routes.astype(jnp.int32), axis=1)
    gates = routed_scale * chosen / jnp.sum(chosen, axis=1, keepdims=True)
    expert_out = routed_rows(hidden, routes, gate_weight, up_weight, down_weight)
    moe_out = jnp.sum(gates[:, :, None] * expert_out.astype(jnp.float32), axis=1).astype(jnp.bfloat16)
    attn_latent = attention(q_latent, q_rope, cache_latent, cache_rope, lengths)
    return (moe_out, attn_latent)
```

```python
import functools

import jax
import jax.numpy as jnp
from jax import lax
from jax.experimental import pallas as pl
from jax.experimental.pallas import tpu as pltpu
from jax.sharding import PartitionSpec as P

MESH = pl.DeviceIdType.MESH
lanes = 128

softmax_scale = 192.0 ** (-0.5)
routed_scale = 2.5


def dispatched(
    hidden,
    routes,
    router_weight,
    gate_weight,
    up_weight,
    down_weight,
    q_latent,
    q_rope,
    cache_latent,
    cache_rope,
    lengths,
):
    token_count, top_count = routes.shape
    expert_count = lax.axis_size("ep")
    capacity = min(token_count, 4 * token_count * top_count // expert_count)
    partial_logits = jnp.dot(hidden, router_weight, preferred_element_type=jnp.float32)
    logits = lax.psum(partial_logits, "tp")
    affinity = jax.nn.sigmoid(logits)
    expert_iota = jnp.arange(expert_count, dtype=jnp.int32)
    chosen_mask = routes[:, :, None] == expert_iota[None, None, :]
    chosen = jnp.sum(jnp.where(chosen_mask, affinity[:, None, :], 0.0), axis=2)
    gates = routed_scale * chosen / jnp.sum(chosen, axis=1, keepdims=True)
    flat_mask = chosen_mask.reshape(token_count * top_count, expert_count).astype(jnp.int32)
    earlier = jnp.cumsum(flat_mask, axis=0) - flat_mask
    within = jnp.sum(flat_mask * earlier, axis=1).reshape(token_count, top_count)
    slot_index = routes * capacity + within
    slot_iota = jnp.arange(expert_count * capacity, dtype=jnp.int32)
    placing = jnp.sum(
        (slot_index[None, :, :] == slot_iota[:, None, None]).astype(jnp.int32), axis=2
    )
    placing = placing.astype(jnp.bfloat16)
    outgoing = jnp.dot(placing, hidden, preferred_element_type=jnp.float32).astype(jnp.bfloat16)
    outgoing = outgoing.reshape(expert_count, capacity, hidden.shape[1])
    received = lax.all_to_all(outgoing, "ep", split_axis=0, concat_axis=0, tiled=True)
    received = lax.all_gather(received, "tp", axis=2, tiled=True)
    source_count, slot_count, feature_count = received.shape
    flat_rows = received.reshape(source_count * slot_count, feature_count)
    gate_part = jnp.dot(flat_rows, gate_weight[0], preferred_element_type=jnp.float32)
    up_part = jnp.dot(flat_rows, up_weight[0], preferred_element_type=jnp.float32)
    active = (jax.nn.silu(gate_part) * up_part).astype(jnp.bfloat16)
    partial_out = jnp.dot(active, down_weight[0], preferred_element_type=jnp.float32)
    summed = lax.psum_scatter(partial_out, "tp", scatter_dimension=1, tiled=True).astype(
        jnp.bfloat16
    )
    summed = summed.reshape(source_count, slot_count, summed.shape[1])
    returned = lax.all_to_all(summed, "ep", split_axis=0, concat_axis=0, tiled=True)
    scores = jnp.einsum("bhl,bjl->bhj", q_latent, cache_latent, preferred_element_type=jnp.float32)
    scores = scores + jnp.einsum(
        "bhr,brj->bhj", q_rope, cache_rope, preferred_element_type=jnp.float32
    )
    scores = scores * softmax_scale
    position = jnp.arange(cache_latent.shape[1], dtype=jnp.int32)
    live = position[None, None, :] < lengths[:, None, None]
    scores = jnp.where(live, scores, -jnp.inf)
    highest = jnp.max(scores, axis=2, keepdims=True)
    expo = jnp.where(live, jnp.exp(scores - highest), 0.0)
    attn_probs = (expo / jnp.sum(expo, axis=2, keepdims=True)).astype(jnp.bfloat16)
    attn_latent = jnp.einsum(
        "bhj,bjl->bhl", attn_probs, cache_latent, preferred_element_type=jnp.float32
    )
    attn_latent = attn_latent.astype(jnp.bfloat16)
    returned_flat = returned.reshape(expert_count * capacity, returned.shape[2])
    picked = jnp.take(returned_flat, slot_index.reshape(-1), axis=0).reshape(
        token_count, top_count, returned.shape[2]
    )
    moe_out = jnp.sum(gates[:, :, None] * picked.astype(jnp.float32), axis=1).astype(jnp.bfloat16)
    return (moe_out, attn_latent)


def fused_kernel(
    columns,
    hidden,
    routes,
    router_weight,
    gate_weight,
    up_weight,
    down_weight,
    q_latent,
    q_rope,
    cache_latent,
    cache_rope,
    lengths,
    moe_out,
    attn_out,
    rows_all,
    routes_v,
    router_v,
    gate_v,
    up_v,
    down_v,
    q_v,
    qr_v,
    cl_v,
    cr_v,
    logit_v,
    act_v,
    tp_out,
    tp_in,
    y_out,
    y_in,
    keep,
    z_out,
    z_in,
    load_sem,
    up_send,
    down_send,
    cross_send,
    core_send,
    line_recv,
    cross_recv,
    core_recv,
    logit_sem,
    tp_sem,
    y_sem,
    z_send,
    z_recv,
):
    tokens, features = hidden.shape
    experts = rows_all.shape[1] // tokens
    line = experts // 2
    chunks = features // columns
    me = lax.axis_index("ep")
    core = lax.axis_index("tp")
    other = 1 - core
    z = me // 2
    y = me % 2
    across = me + 1 - 2 * y

    def rows_of(s, side):
        return pl.ds(pl.multiple_of((s * 2 + side) * tokens, tokens), tokens)

    local_loads = [
        (hidden, rows_all.at[core, rows_of(z, y), pl.ds(0, features)]),
        (routes, routes_v),
        (q_latent, q_v),
        (q_rope, qr_v),
        (cache_latent, cl_v),
        (cache_rope, cr_v),
        (router_weight, router_v),
        (gate_weight.at[0, pl.ds(0, features), :], gate_v.at[0]),
        (gate_weight.at[0, pl.ds(features, features), :], gate_v.at[1]),
        (up_weight.at[0, pl.ds(0, features), :], up_v.at[0]),
        (up_weight.at[0, pl.ds(features, features), :], up_v.at[1]),
        (down_weight.at[0, :, pl.ds(0, features)], down_v.at[0]),
        (down_weight.at[0, :, pl.ds(features, features)], down_v.at[1]),
    ]
    loads = [
        pltpu.make_async_copy(src, dst, load_sem.at[i]) for i, (src, dst) in enumerate(local_loads)
    ]
    for load in loads:
        load.start()

    barrier = pltpu.get_barrier_semaphore()
    pl.semaphore_signal(barrier, inc=1, device_id={"tp": other}, device_id_type=MESH)
    pl.semaphore_signal(barrier, inc=1, device_id={"ep": across}, device_id_type=MESH)
    for d in range(1, line):
        pl.semaphore_signal(
            barrier, inc=1, device_id={"ep": ((z + d) % line) * 2 + y}, device_id_type=MESH
        )

    loads[1].wait()
    expert_lane = lax.broadcasted_iota(jnp.int32, (tokens, lanes), 1)
    chosen_mask = jnp.zeros((tokens, lanes), jnp.float32)
    for k in range(routes.shape[1]):
        chosen_mask += (routes_v[:, k : k + 1] == expert_lane).astype(jnp.float32)
    rows_all[core, rows_of(z, y), features:] = chosen_mask.astype(jnp.bfloat16)
    loads[0].wait()
    pl.semaphore_wait(barrier, line + 1)

    def rows_copy(s, side, send_sem, recv_sem, device):
        block = rows_all.at[core, rows_of(s, side), :]
        return pltpu.make_async_remote_copy(
            src_ref=block,
            dst_ref=block,
            send_sem=send_sem,
            recv_sem=recv_sem,
            device_id=device,
            device_id_type=MESH,
        )

    def to_up(s):
        return rows_copy(s, y, up_send.at[s], line_recv.at[s], {"ep": me + 2})

    def to_down(s):
        return rows_copy(s, y, down_send.at[s], line_recv.at[s], {"ep": me - 2})

    def to_across(s):
        return rows_copy(s, y, cross_send.at[s], cross_recv.at[s], {"ep": across})

    def from_across(s):
        return rows_copy(s, 1 - y, cross_send.at[s], cross_recv.at[s], {"ep": across})

    def to_core(s, side):
        index = s * 2 + side
        return rows_copy(s, side, core_send.at[index], core_recv.at[index], {"tp": other})

    def from_core(index):
        block = rows_all.at[other, pl.ds(index * tokens, tokens), :]
        return pltpu.make_async_remote_copy(
            src_ref=block,
            dst_ref=block,
            send_sem=core_send.at[index],
            recv_sem=core_recv.at[index],
            device_id={"tp": other},
            device_id_type=MESH,
        )

    def attend(b):
        scores = lax.dot_general(
            q_v[b], cl_v[b], (((1,), (1,)), ((), ())), preferred_element_type=jnp.float32
        )
        scores += jnp.dot(qr_v[b], cr_v[b], preferred_element_type=jnp.float32)
        scores *= softmax_scale
        live = lax.broadcasted_iota(jnp.int32, scores.shape, 1) < lengths[b]
        scores = jnp.where(live, scores, -jnp.inf)
        highest = jnp.max(scores, axis=1, keepdims=True)
        expo = jnp.where(live, jnp.exp(scores - highest), 0.0)
        probs = (expo / jnp.sum(expo, axis=1, keepdims=True)).astype(jnp.bfloat16)
        mixed = jnp.dot(probs, cl_v[b], preferred_element_type=jnp.float32)
        attn_out[b] = mixed.astype(attn_out.dtype)

    can_up = z < line - 1
    can_down = z > 0
    pl.when(can_up)(lambda: to_up(z).start())
    pl.when(can_down)(lambda: to_down(z).start())
    to_across(z).start()
    to_core(z, y).start()

    for load in loads[2:6]:
        load.wait()
    seqs = q_v.shape[0]
    for r in range(1, line + 1):
        for b in range(seqs * (r - 1) // line, seqs * r // line):
            attend(b)
        if r < line:

            @pl.when(z >= r)
            def _():
                s = z - r
                to_up(s).wait_recv()
                pl.when(can_up)(lambda: to_up(s).start())
                to_across(s).start()
                to_core(s, y).start()

            @pl.when(z + r < line)
            def _():
                s = z + r
                to_down(s).wait_recv()
                pl.when(can_down)(lambda: to_down(s).start())
                to_across(s).start()
                to_core(s, y).start()

        def crossed(s):
            from_across(s).wait_recv()
            to_core(s, 1 - y).start()

        if r == 1:
            crossed(z)
        else:
            pl.when(z >= r - 1)(lambda: crossed(z - (r - 1)))
            pl.when(z + r - 1 < line)(lambda: crossed(z + r - 1))

    loads[6].wait()
    own = rows_all[core, :, :features]
    logit_v[0] = jnp.zeros(logit_v.shape[1:], jnp.float32)
    logit_v[0, :, :experts] = jnp.dot(own, router_v[...], preferred_element_type=jnp.float32)
    logit_copy = pltpu.make_async_remote_copy(
        src_ref=logit_v.at[0],
        dst_ref=logit_v.at[1],
        send_sem=logit_sem.at[0],
        recv_sem=logit_sem.at[1],
        device_id={"tp": other},
        device_id_type=MESH,
    )
    logit_copy.start()

    for load in loads[7:11]:
        load.wait()
    gate_part = jnp.dot(own, gate_v[core], preferred_element_type=jnp.float32)
    up_part = jnp.dot(own, up_v[core], preferred_element_type=jnp.float32)
    for index in range(experts):
        from_core(index).wait_recv()
    theirs = rows_all[other, :, :features]
    gate_part += jnp.dot(theirs, gate_v[other], preferred_element_type=jnp.float32)
    up_part += jnp.dot(theirs, up_v[other], preferred_element_type=jnp.float32)
    act_v[...] = (gate_part / (1.0 + jnp.exp(-gate_part)) * up_part).astype(jnp.bfloat16)

    logit_copy.wait_recv()
    affinity = 1.0 / (1.0 + jnp.exp(-(logit_v[0] + logit_v[1])))
    chosen = affinity * rows_all[core, :, features:].astype(jnp.float32)
    expert_lane = lax.broadcasted_iota(jnp.int32, chosen.shape, 1)
    mine = jnp.sum(jnp.where(expert_lane == me, chosen, 0.0), axis=1, keepdims=True)
    gate = routed_scale * mine / jnp.sum(chosen, axis=1, keepdims=True)

    for load in loads[11:]:
        load.wait()

    def tp_copy(j):
        return pltpu.make_async_remote_copy(
            src_ref=tp_out.at[j],
            dst_ref=tp_in.at[j],
            send_sem=tp_sem.at[0, j],
            recv_sem=tp_sem.at[1, j],
            device_id={"tp": other},
            device_id_type=MESH,
        )

    def y_copy(j):
        return pltpu.make_async_remote_copy(
            src_ref=y_out.at[j],
            dst_ref=y_in.at[j],
            send_sem=y_sem.at[0, j],
            recv_sem=y_sem.at[1, j],
            device_id={"ep": across},
            device_id_type=MESH,
        )

    def z_copy(j, d):
        target = (z + d) % line
        return pltpu.make_async_remote_copy(
            src_ref=z_out.at[j, target],
            dst_ref=z_in.at[j, d - 1],
            send_sem=z_send.at[j, d - 1],
            recv_sem=z_recv.at[j, d - 1],
            device_id={"ep": target * 2 + y},
            device_id_type=MESH,
        )

    def expert_columns(half, j):
        part = jnp.dot(
            act_v[...],
            down_v[half, :, j * columns : (j + 1) * columns],
            preferred_element_type=jnp.float32,
        )
        return part * gate

    for j in range(chunks):
        tp_out[j] = expert_columns(other, j).astype(jnp.bfloat16)
        tp_copy(j).start()

    def along_line(j):
        y_copy(j).wait_recv()
        total = keep[j] + y_in[j].astype(jnp.float32)
        keep[j] = total
        z_out[j] = total.astype(jnp.bfloat16)
        for d in range(1, line):
            z_copy(j, d).start()

    lag = 3
    for j in range(chunks):
        part = expert_columns(core, j)
        tp_copy(j).wait_recv()
        part = (part + tp_in[j].astype(jnp.float32)).reshape(line, 2, tokens, columns)
        even, odd = part[:, 0], part[:, 1]
        y_out[j] = jnp.where(y == 0, odd, even).astype(jnp.bfloat16)
        y_copy(j).start()
        keep[j] = jnp.where(y == 0, even, odd)
        if j >= lag:
            along_line(j - lag)
    for j in range(max(chunks - lag, 0), chunks):
        along_line(j)
    for j in range(chunks):
        total = keep[j, z]
        for d in range(1, line):
            z_copy(j, d).wait_recv()
            total += z_in[j, d - 1].astype(jnp.float32)
        moe_out[:, j * columns : (j + 1) * columns] = total.astype(moe_out.dtype)

    for s in range(line):
        pl.when(can_up & (s <= z))(lambda: to_up(s).wait_send())
        pl.when(can_down & (s >= z))(lambda: to_down(s).wait_send())
        to_across(s).wait_send()
        to_core(s, 0).wait_send()
        to_core(s, 1).wait_send()
    logit_copy.wait_send()
    for j in range(chunks):
        tp_copy(j).wait_send()
        y_copy(j).wait_send()
        for d in range(1, line):
            z_copy(j, d).wait_send()


def fused(*operands):
    hidden, routes = operands[:2]
    tokens, features = hidden.shape
    experts = lax.axis_size("ep")
    line = experts // 2
    hidden_units = operands[3].shape[2]
    seqs, heads, latent = operands[6].shape
    rope = operands[7].shape[2]
    cache = operands[8].shape[1]
    columns = 256 if features % 256 == 0 else lanes
    chunks = features // columns
    every = experts * tokens
    bf16, f32 = jnp.bfloat16, jnp.float32
    dma = pltpu.SemaphoreType.DMA
    anywhere = pl.BlockSpec(memory_space=pl.ANY)
    vmem = pl.BlockSpec(memory_space=pltpu.VMEM)
    return pl.pallas_call(
        functools.partial(fused_kernel, columns),
        out_shape=(
            jax.ShapeDtypeStruct((tokens, features), bf16),
            jax.ShapeDtypeStruct((seqs, heads, latent), bf16),
        ),
        in_specs=[anywhere] * 10 + [pl.BlockSpec(memory_space=pltpu.SMEM)],
        out_specs=(vmem, vmem),
        scratch_shapes=[
            pltpu.VMEM((2, every, features + lanes), bf16),
            pltpu.VMEM(routes.shape, jnp.int32),
            pltpu.VMEM(operands[2].shape, bf16),
            pltpu.VMEM((2, features, hidden_units), bf16),
            pltpu.VMEM((2, features, hidden_units), bf16),
            pltpu.VMEM((2, hidden_units, features), bf16),
            pltpu.VMEM((seqs, heads, latent), bf16),
            pltpu.VMEM((seqs, heads, rope), bf16),
            pltpu.VMEM((seqs, cache, latent), bf16),
            pltpu.VMEM((seqs, rope, cache), bf16),
            pltpu.VMEM((2, every, lanes), f32),
            pltpu.VMEM((every, hidden_units), bf16),
            pltpu.VMEM((chunks, every, columns), bf16),
            pltpu.VMEM((chunks, every, columns), bf16),
            pltpu.VMEM((chunks, line, tokens, columns), bf16),
            pltpu.VMEM((chunks, line, tokens, columns), bf16),
            pltpu.VMEM((chunks, line, tokens, columns), f32),
            pltpu.VMEM((chunks, line, tokens, columns), bf16),
            pltpu.VMEM((chunks, line - 1, tokens, columns), bf16),
            dma((13,)),
            dma((line,)),
            dma((line,)),
            dma((line,)),
            dma((experts,)),
            dma((line,)),
            dma((line,)),
            dma((experts,)),
            dma((2,)),
            dma((2, chunks)),
            dma((2, chunks)),
            dma((chunks, line - 1)),
            dma((chunks, line - 1)),
        ],
        compiler_params=pltpu.CompilerParams(
            collective_id=0, has_side_effects=True, vmem_limit_bytes=60 * 1024 * 1024
        ),
    )(*operands)


def local(*operands):
    tokens, top = operands[1].shape
    experts = lax.axis_size("ep")
    capacity = min(tokens, 4 * tokens * top // experts)
    whole_tiles = tokens % 16 == 0 and operands[0].shape[1] % lanes == 0
    if capacity == tokens and lax.axis_size("tp") == 2 and experts % 2 == 0 and whole_tiles:
        if 4 <= experts <= 16:
            return fused(*operands)
    return dispatched(*operands)


def solution(mesh):
    return jax.shard_map(
        local,
        mesh=mesh,
        in_specs=(
            P(("groups", "ep"), "tp"),
            P(("groups", "ep"), None),
            P("tp", None),
            P("ep", None, "tp"),
            P("ep", None, "tp"),
            P("ep", "tp", None),
            P(("groups", "ep"), "tp", None),
            P(("groups", "ep"), "tp", None),
            P(("groups", "ep"), None, None),
            P(("groups", "ep"), None, None),
            P(("groups", "ep")),
        ),
        out_specs=(P(("groups", "ep"), "tp"), P(("groups", "ep"), "tp", None)),
        check_vma=False,
    )
```

```python
import functools

import jax
import jax.numpy as jnp
from jax import lax
from jax.experimental import pallas as pl
from jax.experimental.pallas import tpu as pltpu
from jax.sharding import PartitionSpec as P

MESH = pl.DeviceIdType.MESH
lanes = 128

softmax_scale = 192.0 ** (-0.5)
routed_scale = 2.5


def dispatched(
    hidden,
    routes,
    router_weight,
    gate_weight,
    up_weight,
    down_weight,
    q_latent,
    q_rope,
    cache_latent,
    cache_rope,
    lengths,
):
    token_count, top_count = routes.shape
    expert_count = lax.axis_size("ep")
    capacity = min(token_count, 4 * token_count * top_count // expert_count)
    partial_logits = jnp.dot(hidden, router_weight, preferred_element_type=jnp.float32)
    logits = lax.psum(partial_logits, "tp")
    affinity = jax.nn.sigmoid(logits)
    expert_iota = jnp.arange(expert_count, dtype=jnp.int32)
    chosen_mask = routes[:, :, None] == expert_iota[None, None, :]
    chosen = jnp.sum(jnp.where(chosen_mask, affinity[:, None, :], 0.0), axis=2)
    gates = routed_scale * chosen / jnp.sum(chosen, axis=1, keepdims=True)
    flat_mask = chosen_mask.reshape(token_count * top_count, expert_count).astype(jnp.int32)
    earlier = jnp.cumsum(flat_mask, axis=0) - flat_mask
    within = jnp.sum(flat_mask * earlier, axis=1).reshape(token_count, top_count)
    slot_index = routes * capacity + within
    slot_iota = jnp.arange(expert_count * capacity, dtype=jnp.int32)
    placing = jnp.sum(
        (slot_index[None, :, :] == slot_iota[:, None, None]).astype(jnp.int32), axis=2
    )
    placing = placing.astype(jnp.bfloat16)
    outgoing = jnp.dot(placing, hidden, preferred_element_type=jnp.float32).astype(jnp.bfloat16)
    outgoing = outgoing.reshape(expert_count, capacity, hidden.shape[1])
    received = lax.all_to_all(outgoing, "ep", split_axis=0, concat_axis=0, tiled=True)
    received = lax.all_gather(received, "tp", axis=2, tiled=True)
    source_count, slot_count, feature_count = received.shape
    flat_rows = received.reshape(source_count * slot_count, feature_count)
    gate_part = jnp.dot(flat_rows, gate_weight[0], preferred_element_type=jnp.float32)
    up_part = jnp.dot(flat_rows, up_weight[0], preferred_element_type=jnp.float32)
    active = (jax.nn.silu(gate_part) * up_part).astype(jnp.bfloat16)
    partial_out = jnp.dot(active, down_weight[0], preferred_element_type=jnp.float32)
    summed = lax.psum_scatter(partial_out, "tp", scatter_dimension=1, tiled=True).astype(
        jnp.bfloat16
    )
    summed = summed.reshape(source_count, slot_count, summed.shape[1])
    returned = lax.all_to_all(summed, "ep", split_axis=0, concat_axis=0, tiled=True)
    scores = jnp.einsum("bhl,bjl->bhj", q_latent, cache_latent, preferred_element_type=jnp.float32)
    scores = scores + jnp.einsum(
        "bhr,brj->bhj", q_rope, cache_rope, preferred_element_type=jnp.float32
    )
    scores = scores * softmax_scale
    position = jnp.arange(cache_latent.shape[1], dtype=jnp.int32)
    live = position[None, None, :] < lengths[:, None, None]
    scores = jnp.where(live, scores, -jnp.inf)
    highest = jnp.max(scores, axis=2, keepdims=True)
    expo = jnp.where(live, jnp.exp(scores - highest), 0.0)
    attn_probs = (expo / jnp.sum(expo, axis=2, keepdims=True)).astype(jnp.bfloat16)
    attn_latent = jnp.einsum(
        "bhj,bjl->bhl", attn_probs, cache_latent, preferred_element_type=jnp.float32
    )
    attn_latent = attn_latent.astype(jnp.bfloat16)
    returned_flat = returned.reshape(expert_count * capacity, returned.shape[2])
    picked = jnp.take(returned_flat, slot_index.reshape(-1), axis=0).reshape(
        token_count, top_count, returned.shape[2]
    )
    moe_out = jnp.sum(gates[:, :, None] * picked.astype(jnp.float32), axis=1).astype(jnp.bfloat16)
    return (moe_out, attn_latent)


def fused_kernel(
    columns,
    parts,
    hidden,
    routes,
    router_weight,
    gate_weight,
    up_weight,
    down_weight,
    q_latent,
    q_rope,
    cache_latent,
    cache_rope,
    lengths,
    moe_out,
    attn_out,
    rows_all,
    routes_v,
    router_v,
    gate_v,
    up_v,
    down_v,
    q_v,
    qr_v,
    cl_v,
    cr_v,
    logit_v,
    act_v,
    tp_out,
    tp_in,
    y_out,
    y_in,
    keep,
    z_out,
    z_in,
    load_sem,
    up_send,
    down_send,
    cross_send,
    core_send,
    line_recv,
    cross_recv,
    core_recv,
    logit_sem,
    tp_sem,
    y_sem,
    z_send,
    z_recv,
):
    tokens, features = hidden.shape
    experts = rows_all.shape[1] // tokens
    line = experts // 2
    chunks = features // columns
    me = lax.axis_index("ep")
    core = lax.axis_index("tp")
    other = 1 - core
    z = me // 2
    y = me % 2
    across = me + 1 - 2 * y

    def rows_of(s, side):
        return pl.ds(pl.multiple_of((s * 2 + side) * tokens, tokens), tokens)

    local_loads = [
        (hidden, rows_all.at[core, rows_of(z, y), pl.ds(0, features)]),
        (routes, routes_v),
        (q_latent, q_v),
        (q_rope, qr_v),
        (cache_latent, cl_v),
        (cache_rope, cr_v),
        (router_weight, router_v),
        (gate_weight.at[0, pl.ds(0, features), :], gate_v.at[0]),
        (gate_weight.at[0, pl.ds(features, features), :], gate_v.at[1]),
        (up_weight.at[0, pl.ds(0, features), :], up_v.at[0]),
        (up_weight.at[0, pl.ds(features, features), :], up_v.at[1]),
        (down_weight.at[0, :, pl.ds(0, features)], down_v.at[0]),
        (down_weight.at[0, :, pl.ds(features, features)], down_v.at[1]),
    ]
    loads = [
        pltpu.make_async_copy(src, dst, load_sem.at[i]) for i, (src, dst) in enumerate(local_loads)
    ]
    for load in loads:
        load.start()

    barrier = pltpu.get_barrier_semaphore()
    pl.semaphore_signal(barrier, inc=1, device_id={"tp": other}, device_id_type=MESH)
    pl.semaphore_signal(barrier, inc=1, device_id={"ep": across}, device_id_type=MESH)
    can_up = z < line - 1
    can_down = z > 0

    def greet(target):
        pl.semaphore_signal(barrier, inc=1, device_id={"ep": target}, device_id_type=MESH)

    pl.when(can_up)(lambda: greet(me + 2))
    pl.when(can_down)(lambda: greet(me - 2))

    loads[1].wait()
    token_row = lax.broadcasted_iota(jnp.int32, (tokens, lanes), 0)
    token_lane = lax.broadcasted_iota(jnp.int32, (tokens, lanes), 1)
    place = (token_lane == token_row + me * tokens).astype(jnp.bfloat16)
    spread = jnp.dot(
        routes_v[...].astype(jnp.float32).astype(jnp.bfloat16),
        place,
        preferred_element_type=jnp.float32,
    )
    expert_row = token_row.astype(jnp.float32)
    chosen_mask = jnp.zeros((tokens, lanes), jnp.float32)
    for k in range(routes.shape[0]):
        chosen_mask += jnp.where(spread[k : k + 1, :] == expert_row, 1.0, 0.0)
    inside = (token_lane >= me * tokens) & (token_lane < (me + 1) * tokens)
    chosen_mask = jnp.where(inside, chosen_mask, 0.0)
    rows_all[core, rows_of(z, y), features:] = chosen_mask.astype(jnp.bfloat16)
    loads[0].wait()
    inner = can_up & can_down
    pl.when(inner)(lambda: pl.semaphore_wait(barrier, 4))
    pl.when(jnp.logical_not(inner))(lambda: pl.semaphore_wait(barrier, 3))

    width = rows_all.shape[2] // parts

    def rows_copy(half, index, k, send_sem, recv_sem, device):
        rows = pl.ds(pl.multiple_of(index * tokens, tokens), tokens)
        block = rows_all.at[half, rows, pl.ds(k * width, width)]
        return pltpu.make_async_remote_copy(
            src_ref=block,
            dst_ref=block,
            send_sem=send_sem,
            recv_sem=recv_sem,
            device_id=device,
            device_id_type=MESH,
        )

    def to_up(s, k):
        sems = up_send.at[s, k], line_recv.at[s, k]
        return rows_copy(core, s * 2 + y, k, *sems, {"ep": me + 2})

    def to_down(s, k):
        sems = down_send.at[s, k], line_recv.at[s, k]
        return rows_copy(core, s * 2 + y, k, *sems, {"ep": me - 2})

    def to_across(s, k):
        sems = cross_send.at[s, k], cross_recv.at[s, k]
        return rows_copy(core, s * 2 + y, k, *sems, {"ep": across})

    def from_across(s, k):
        sems = cross_send.at[s, k], cross_recv.at[s, k]
        return rows_copy(core, s * 2 + 1 - y, k, *sems, {"ep": across})

    def to_core(index, k):
        sems = core_send.at[index, k], core_recv.at[index, k]
        return rows_copy(core, index, k, *sems, {"tp": other})

    def from_core(index, k):
        sems = core_send.at[index, k], core_recv.at[index, k]
        return rows_copy(other, index, k, *sems, {"tp": other})

    def attend(b):
        scores = lax.dot_general(
            q_v[b], cl_v[b], (((1,), (1,)), ((), ())), preferred_element_type=jnp.float32
        )
        scores += jnp.dot(qr_v[b], cr_v[b], preferred_element_type=jnp.float32)
        scores *= softmax_scale
        live = lax.broadcasted_iota(jnp.int32, scores.shape, 1) < lengths[b]
        scores = jnp.where(live, scores, -jnp.inf)
        highest = jnp.max(scores, axis=1, keepdims=True)
        expo = jnp.where(live, jnp.exp(scores - highest), 0.0)
        probs = (expo / jnp.sum(expo, axis=1, keepdims=True)).astype(jnp.bfloat16)
        mixed = jnp.dot(probs, cl_v[b], preferred_element_type=jnp.float32)
        attn_out[b] = mixed.astype(attn_out.dtype)

    for k in range(parts):
        pl.when(can_up)(lambda: to_up(z, k).start())
        pl.when(can_down)(lambda: to_down(z, k).start())
        to_across(z, k).start()
        to_core(me, k).start()

    for load in loads[2:6]:
        load.wait()
    seqs = q_v.shape[0]
    early = seqs // 2
    for b in range(early):
        attend(b)

    def forward(s, k, ahead, onward):
        onward(s, k).wait_recv()
        pl.when(ahead)(lambda: onward(s, k).start())
        to_across(s, k).start()
        to_core(s * 2 + y, k).start()

    def crossed(s, k):
        from_across(s, k).wait_recv()
        to_core(s * 2 + 1 - y, k).start()

    for r in range(1, line + 1):
        for k in range(parts):
            if r < line:
                pl.when(z >= r)(lambda: forward(z - r, k, can_up, to_up))
                pl.when(z + r < line)(lambda: forward(z + r, k, can_down, to_down))
            if r == 1:
                crossed(z, k)
            else:
                pl.when(z >= r - 1)(lambda: crossed(z - (r - 1), k))
                pl.when(z + r - 1 < line)(lambda: crossed(z + r - 1, k))

    loads[6].wait()
    own = rows_all[core, :, :features]
    logit_v[0] = lax.dot_general(
        router_v[...], own, (((1,), (1,)), ((), ())), preferred_element_type=jnp.float32
    )
    logit_copy = pltpu.make_async_remote_copy(
        src_ref=logit_v.at[0],
        dst_ref=logit_v.at[1],
        send_sem=logit_sem.at[0],
        recv_sem=logit_sem.at[1],
        device_id={"tp": other},
        device_id_type=MESH,
    )
    logit_copy.start()

    for load in loads[7:11]:
        load.wait()
    gate_part = jnp.dot(own, gate_v[core], preferred_element_type=jnp.float32)
    up_part = jnp.dot(own, up_v[core], preferred_element_type=jnp.float32)
    for index in range(experts):
        for k in range(parts):
            from_core(index, k).wait_recv()
    theirs = rows_all[other, :, :features]
    gate_part += jnp.dot(theirs, gate_v[other], preferred_element_type=jnp.float32)
    up_part += jnp.dot(theirs, up_v[other], preferred_element_type=jnp.float32)
    act_v[...] = (gate_part / (1.0 + jnp.exp(-gate_part)) * up_part).astype(jnp.bfloat16)

    logit_copy.wait_recv()
    affinity = 1.0 / (1.0 + jnp.exp(-(logit_v[0] + logit_v[1])))
    masks = rows_all[core, :, features:].astype(jnp.float32).reshape(experts, tokens, lanes)
    chosen = affinity * jnp.sum(masks, axis=0)[:experts]
    expert_row = lax.broadcasted_iota(jnp.int32, chosen.shape, 0)
    mine = jnp.sum(jnp.where(expert_row == me, chosen, 0.0), axis=0, keepdims=True)
    gate_row = routed_scale * mine / jnp.sum(chosen, axis=0, keepdims=True)
    gate = jnp.transpose(jnp.broadcast_to(gate_row, (lanes, lanes)))[:, :1]

    for load in loads[11:]:
        load.wait()

    def tp_copy(j):
        return pltpu.make_async_remote_copy(
            src_ref=tp_out.at[j],
            dst_ref=tp_in.at[j],
            send_sem=tp_sem.at[0, j],
            recv_sem=tp_sem.at[1, j],
            device_id={"tp": other},
            device_id_type=MESH,
        )

    def y_copy(j):
        return pltpu.make_async_remote_copy(
            src_ref=y_out.at[j],
            dst_ref=y_in.at[j],
            send_sem=y_sem.at[0, j],
            recv_sem=y_sem.at[1, j],
            device_id={"ep": across},
            device_id_type=MESH,
        )

    def z_copy(j, d):
        target = (z + d) % line
        return pltpu.make_async_remote_copy(
            src_ref=z_out.at[j, target],
            dst_ref=z_in.at[j, d - 1],
            send_sem=z_send.at[j, d - 1],
            recv_sem=z_recv.at[j, d - 1],
            device_id={"ep": target * 2 + y},
            device_id_type=MESH,
        )

    def expert_columns(half, j):
        part = jnp.dot(
            act_v[...],
            down_v[half, :, j * columns : (j + 1) * columns],
            preferred_element_type=jnp.float32,
        )
        return part * gate

    for j in range(chunks):
        tp_out[j] = expert_columns(other, j).astype(jnp.bfloat16)
        tp_copy(j).start()

    def along_line(j):
        y_copy(j).wait_recv()
        total = keep[j] + y_in[j].astype(jnp.float32)
        keep[j] = total
        z_out[j] = total.astype(jnp.bfloat16)
        for d in range(1, line):
            z_copy(j, d).start()

    lag = chunks
    for j in range(chunks):
        part = expert_columns(core, j)
        tp_copy(j).wait_recv()
        part = (part + tp_in[j].astype(jnp.float32)).reshape(line, 2, tokens, columns)
        even, odd = part[:, 0], part[:, 1]
        y_out[j] = jnp.where(y == 0, odd, even).astype(jnp.bfloat16)
        y_copy(j).start()
        keep[j] = jnp.where(y == 0, even, odd)
        if j >= lag:
            along_line(j - lag)
    for j in range(max(chunks - lag, 0), chunks):
        along_line(j)
    for b in range(early, seqs):
        attend(b)
    for j in range(chunks):
        total = keep[j, z]
        for d in range(1, line):
            z_copy(j, d).wait_recv()
            total += z_in[j, d - 1].astype(jnp.float32)
        moe_out[:, j * columns : (j + 1) * columns] = total.astype(moe_out.dtype)

    for s in range(line):
        for k in range(parts):
            pl.when(can_up & (s <= z))(lambda: to_up(s, k).wait_send())
            pl.when(can_down & (s >= z))(lambda: to_down(s, k).wait_send())
            to_across(s, k).wait_send()
            to_core(s * 2, k).wait_send()
            to_core(s * 2 + 1, k).wait_send()
    logit_copy.wait_send()
    for j in range(chunks):
        tp_copy(j).wait_send()
        y_copy(j).wait_send()
        for d in range(1, line):
            z_copy(j, d).wait_send()


def fused(hidden, routes, router_weight, *others):
    operands = (hidden, routes.T, router_weight.T) + others
    routes = operands[1]
    tokens, features = hidden.shape
    experts = lax.axis_size("ep")
    line = experts // 2
    hidden_units = operands[3].shape[2]
    seqs, heads, latent = operands[6].shape
    rope = operands[7].shape[2]
    cache = operands[8].shape[1]
    columns = 256 if features % 256 == 0 else lanes
    chunks = features // columns
    parts = 3 if (features // lanes + 1) % 3 == 0 else 1
    every = experts * tokens
    bf16, f32 = jnp.bfloat16, jnp.float32
    dma = pltpu.SemaphoreType.DMA
    in_hbm = pl.BlockSpec(memory_space=pltpu.HBM)
    vmem = pl.BlockSpec(memory_space=pltpu.VMEM)
    return pl.pallas_call(
        functools.partial(fused_kernel, columns, parts),
        out_shape=(
            jax.ShapeDtypeStruct((tokens, features), bf16),
            jax.ShapeDtypeStruct((seqs, heads, latent), bf16),
        ),
        in_specs=[in_hbm] * 10 + [pl.BlockSpec(memory_space=pltpu.SMEM)],
        out_specs=(vmem, vmem),
        scratch_shapes=[
            pltpu.VMEM((2, every, features + lanes), bf16),
            pltpu.VMEM(routes.shape, jnp.int32),
            pltpu.VMEM(operands[2].shape, bf16),
            pltpu.VMEM((2, features, hidden_units), bf16),
            pltpu.VMEM((2, features, hidden_units), bf16),
            pltpu.VMEM((2, hidden_units, features), bf16),
            pltpu.VMEM((seqs, heads, latent), bf16),
            pltpu.VMEM((seqs, heads, rope), bf16),
            pltpu.VMEM((seqs, cache, latent), bf16),
            pltpu.VMEM((seqs, rope, cache), bf16),
            pltpu.VMEM((2, experts, lanes), f32),
            pltpu.VMEM((every, hidden_units), bf16),
            pltpu.VMEM((chunks, every, columns), bf16),
            pltpu.VMEM((chunks, every, columns), bf16),
            pltpu.VMEM((chunks, line, tokens, columns), bf16),
            pltpu.VMEM((chunks, line, tokens, columns), bf16),
            pltpu.VMEM((chunks, line, tokens, columns), f32),
            pltpu.VMEM((chunks, line, tokens, columns), bf16),
            pltpu.VMEM((chunks, line - 1, tokens, columns), bf16),
            dma((13,)),
            dma((line, parts)),
            dma((line, parts)),
            dma((line, parts)),
            dma((experts, parts)),
            dma((line, parts)),
            dma((line, parts)),
            dma((experts, parts)),
            dma((2,)),
            dma((2, chunks)),
            dma((2, chunks)),
            dma((chunks, line - 1)),
            dma((chunks, line - 1)),
        ],
        compiler_params=pltpu.CompilerParams(
            collective_id=0, has_side_effects=True, vmem_limit_bytes=60 * 1024 * 1024
        ),
    )(*operands)


def local(*operands):
    tokens, top = operands[1].shape
    experts = lax.axis_size("ep")
    capacity = min(tokens, 4 * tokens * top // experts)
    whole_tiles = tokens % 16 == 0 and operands[0].shape[1] % lanes == 0
    if capacity == tokens and lax.axis_size("tp") == 2 and experts % 2 == 0 and whole_tiles:
        if experts in (4, 8) and experts * tokens == lanes:
            return fused(*operands)
    return dispatched(*operands)


def solution(mesh):
    return jax.shard_map(
        local,
        mesh=mesh,
        in_specs=(
            P(("groups", "ep"), "tp"),
            P(("groups", "ep"), None),
            P("tp", None),
            P("ep", None, "tp"),
            P("ep", None, "tp"),
            P("ep", "tp", None),
            P(("groups", "ep"), "tp", None),
            P(("groups", "ep"), "tp", None),
            P(("groups", "ep"), None, None),
            P(("groups", "ep"), None, None),
            P(("groups", "ep")),
        ),
        out_specs=(P(("groups", "ep"), "tp"), P(("groups", "ep"), "tp", None)),
        check_vma=False,
    )
```
